32 devices in a mesh: kpt: 2 (over y), row: 8 (over z, x), freq: 2 (over core).
Axes of the slice: x: 2, y: 2, z: 4, core: 2. Of those that a mesh axis runs over, the one named last changes fastest.
Arguments:
- screened: bfloat16 [8, 2, 8192, 8192], P(('kpt', 'freq'), None, 'row'), parts along dimension 0, may hold values from -0.0625 to 0.0625
- elements: bfloat16 [2, 1024, 8192], P(None, 'kpt', 'row'), parts along dimension 1, may hold values from -0.59765625 to 0.59765625
- node_freq: float32 [4], P('freq'), may hold values from 0.1 to 2
- node_weight: float32 [4], P('freq'), may hold values from 0.1 to 1
- band_energy: float32 [1024], P('kpt'), parts along dimension 0, may hold values from -1 to 1
- energy_grid: float32 [64], replicated, may hold values from -1 to 1
- pair_state: int32 [1024], P('kpt'), parts along dimension 0, may hold values from 0 to 31
- pair_band: int32 [1024], P('kpt'), parts along dimension 0, may hold values from 0 to 511
Outputs:
- sigma: float32 [2, 64, 64], P(None, 'kpt'), parts along dimension 1
The draws below stay inside these ranges and needn't reach their ends.
There are 2 independent parts, one for each index of `kpt`. The reference program is written for one: setup_inputs(seed, part) draws one part's arguments, and reference() takes and returns one part's arrays. A program takes and returns all parts, laid end to end along the dimension named above; an argument that names none is the same for every part. Nothing has to cross between parts.
All inputs are finite; a program needn't handle non-finite values.
Results may differ from the reference program's by a relative error of at most 0.0003.
Values may be sent and summed in bfloat16 or wider, within the bound.
A program may use at most 192 MiB of HBM per device.

```python
import math
import jax
import jax.numpy as jnp

NG = 8192
NPAIR = 512
NBAND = 512
NSTATE = 32
NE = 64
NODES = 4


def place_ends(result, key, low, largest):
    spot = [jax.random.randint(jax.random.fold_in(key, axis), (), 0, length) for axis, length in enumerate(result.shape)]
    main_axis = result.shape.index(max(result.shape))
    neighbour = spot[:main_axis] + [(spot[main_axis] + 1) % result.shape[main_axis]] + spot[main_axis + 1:]
    return result.at[tuple(spot)].set(low).at[tuple(neighbour)].set(largest)


def steps_of(own_key, shape, split, low, high):
    def one(dim, shards_of):
        steps = jax.random.uniform(jax.random.fold_in(jax.random.fold_in(own_key, 6), dim), (shards_of,), jnp.float32, low / len(split), high / len(split))
        return jnp.repeat(jnp.exp(steps), shape[dim] // shards_of).reshape((-1,) + (1,) * (len(shape) - dim - 1))

    loudness = one(*split[0])
    for cut in split[1:]:
        loudness = loudness * one(*cut)
    return loudness


def centred(key, extent, scale, most, shards=(), kind=jnp.bfloat16):
    result = scale * jax.random.normal(key, extent, jnp.float32)
    if shards:
        result = result * steps_of(key, extent, shards, -0.22, 0.18)
    return jnp.clip(result, -most, most).astype(kind)


def setup_inputs(seed: int = 0, part: int = 0) -> dict:
    key_of = jax.random.split(jax.random.key(seed), 9)
    part_splits = jax.random.split(jax.random.fold_in(key_of[8], part), 9)
    return {
        "screened": centred(part_splits[0], (NODES, 2, NG, NG), NG ** -0.5, 0.0625, ((0, 2), (2, 8))),
        "elements": centred(part_splits[1], (2, NPAIR, NG), 0.1, 0.59765625, ((2, 8),)),
        "node_freq": jnp.clip(jnp.exp(math.log(2.0) - 2.9957323 * jax.random.uniform(key_of[2], (NODES,), jnp.float32) ** steps_of(key_of[2], (NODES,), ((0, 2),), -0.2, 0.2)), 0.1, 2.0),
        "node_weight": jnp.clip(jnp.exp(math.log(1.0) - 2.3025851 * jax.random.uniform(key_of[3], (NODES,), jnp.float32) ** steps_of(key_of[3], (NODES,), ((0, 2),), -0.2, 0.2)), 0.1, 1.0),
        "band_energy": jnp.clip(jax.random.uniform(part_splits[4], (NBAND,), jnp.float32, -1.0, 1.0), -1.0, 1.0),
        "energy_grid": jnp.clip(jax.random.uniform(key_of[5], (NE,), jnp.float32, -1.0, 1.0), -1.0, 1.0),
        "pair_state": place_ends(jax.random.randint(part_splits[6], (NPAIR,), 0, NSTATE), jax.random.fold_in(part_splits[6], 1), 0, NSTATE - 1).astype(jnp.int32),
        "pair_band": place_ends(jax.random.randint(part_splits[7], (NPAIR,), 0, NBAND), jax.random.fold_in(part_splits[7], 1), 0, NBAND - 1).astype(jnp.int32),
    }


def reference(screened, elements, node_freq, node_weight, band_energy, energy_grid, pair_state, pair_band):
    real_el = elements[0]
    imag_el = elements[1]
    real_t = real_el.T.astype(jnp.float32)
    imag_t = imag_el.T.astype(jnp.float32)
    forms_re = []
    forms_im = []
    for node in range(NODES):
        w_real = screened[node, 0]
        w_imag = screened[node, 1]
        y_real = jnp.dot(w_real, real_el.T, preferred_element_type=jnp.float32) - jnp.dot(w_imag, imag_el.T, preferred_element_type=jnp.float32)
        y_imag = jnp.dot(w_real, imag_el.T, preferred_element_type=jnp.float32) + jnp.dot(w_imag, real_el.T, preferred_element_type=jnp.float32)
        forms_re.append(jnp.sum(real_t * y_real + imag_t * y_imag, axis=0))
        forms_im.append(jnp.sum(real_t * y_imag - imag_t * y_real, axis=0))
    form_re = jnp.stack(forms_re)
    form_im = jnp.stack(forms_im)
    pair_eps = band_energy[pair_band]
    delta = energy_grid[None, :] - pair_eps[:, None]
    factor = node_weight[:, None, None] * delta[None] / (delta[None] ** 2 + node_freq[:, None, None] ** 2)
    terms_re = jnp.sum(form_re[:, :, None] * factor, axis=0)
    terms_im = jnp.sum(form_im[:, :, None] * factor, axis=0)
    sig_re = jax.ops.segment_sum(terms_re, pair_state, NSTATE)
    sig_im = jax.ops.segment_sum(terms_im, pair_state, NSTATE)
    return jnp.stack([sig_re, sig_im])
```

```python
import functools

import jax
import jax.numpy as jnp
from jax import lax
from jax.experimental import pallas as pl
from jax.experimental.pallas import tpu as pltpu
from jax.sharding import PartitionSpec as P

NSTATE = 32
LANES = 256
ROWS = 64
MESH = pl.DeviceIdType.MESH
NT = (((1,), (1,)), ((), ()))


def product(weights, piece):
    return jnp.einsum("jgc,pc->jgp", weights, piece, preferred_element_type=jnp.float32)


def self_energy(
    form_re, form_im, node_freq, node_weight, band_energy, energy_grid, pair_state, pair_band
):
    band_onehot = (
        pair_band[:, None] == jnp.arange(band_energy.shape[0], dtype=jnp.int32)[None, :]
    ).astype(jnp.float32)
    pair_eps = jnp.dot(band_onehot, band_energy, precision=lax.Precision.HIGHEST)
    delta = energy_grid[None, :] - pair_eps[:, None]
    factor = (
        node_weight[:, None, None]
        * delta[None]
        / (delta[None] ** 2 + node_freq[:, None, None] ** 2)
    )
    terms_re = jnp.sum(form_re[:, :, None] * factor, axis=0)
    terms_im = jnp.sum(form_im[:, :, None] * factor, axis=0)
    state_onehot = (jnp.arange(NSTATE, dtype=jnp.int32)[:, None] == pair_state[None, :]).astype(
        jnp.float32
    )
    sig_re = jnp.dot(state_onehot, terms_re, precision=lax.Precision.HIGHEST)
    sig_im = jnp.dot(state_onehot, terms_im, precision=lax.Precision.HIGHEST)
    return jnp.stack([sig_re, sig_im])


def ring_position(idx, n):
    par = idx % 2
    return (1 - par) * (idx // 2) + par * (n - 1 - idx // 2)


def ring_index(pos, n):
    high = pos // (n // 2)
    return (1 - high) * (2 * pos) + high * (2 * (n - 1 - pos) + 1)


def thirds(x):
    high = x.astype(jnp.bfloat16)
    rest = x - high.astype(jnp.float32)
    mid = rest.astype(jnp.bfloat16)
    low = (rest - mid.astype(jnp.float32)).astype(jnp.bfloat16)
    return high, mid, low


def forms_kernel(
    n, nodes, npair, block, lanes, lines,
    w_hbm, m_hbm, freq_hbm, weight_hbm, band_hbm, grid_hbm, state_hbm, pband_hbm,
    out_ref,
    lhs, held, wbuf, zbuf, acc, factor, onehot, forms, peers, twin,
    freq_v, weight_v, band_v, grid_v, state_v, pband_v,
    small_sem, lhs_sem, own_sem, other_sem, w_sem,
    send_sem, recv_sem, sib_send, sib_recv, form_send, form_recv, twin_send, twin_recv,
):
    me = lax.axis_index("row")
    core = lax.axis_index("freq")
    pos = ring_position(me, n)
    right = ring_index((pos + 1) % n, n)
    left = ring_index((pos + n - 1) % n, n)
    other = 1 - core
    half = npair // 2
    subs = block // lanes // 2
    rounds = n * subs

    def item(step, way, hop):
        first = (step + 1) % 2
        owner_pos = (pos + n + (2 * way - 1) * hop) % n
        part = (1 - way) * first + way * (1 - first)
        return ring_index(owner_pos, n), part

    def piece_of(rnd, way):
        step = rnd // subs
        owner, part = item(step, way, (step + 1) // 2)
        return owner, part * subs + rnd % subs

    def w_copies(rnd):
        copies = []
        for way in range(2):
            owner, q = piece_of(rnd, way)
            start = pl.multiple_of(owner * block + q * lanes, 128)
            for j in range(nodes):
                for c in range(2):
                    copies.append(
                        pltpu.make_async_copy(
                            w_hbm.at[j, c, :, pl.ds(start, lanes)],
                            wbuf.at[rnd % 2, way, pl.ds(c * block, block), pl.ds(j * lanes, lanes)],
                            w_sem.at[rnd % 2, way, j, c],
                        )
                    )
        return copies

    def send(rnd, way, owner, q):
        ref = held.at[owner, q, core]
        return pltpu.make_async_remote_copy(
            src_ref=ref,
            dst_ref=ref,
            send_sem=send_sem.at[rnd, way],
            recv_sem=recv_sem.at[rnd, way],
            device_id={"row": right if way == 0 else left},
            device_id_type=MESH,
        )

    def pass_over(rnd, way, owner, q, core_of):
        ref = held.at[owner, q, core_of]
        return pltpu.make_async_remote_copy(
            src_ref=ref,
            dst_ref=ref,
            send_sem=sib_send.at[rnd, way],
            recv_sem=sib_recv.at[rnd, way],
            device_id={"freq": other},
            device_id_type=MESH,
        )

    def own_copy(q, f, sem):
        return pltpu.make_async_copy(
            m_hbm.at[
                :,
                pl.ds(pl.multiple_of(f * half, half), half),
                pl.ds(q * lanes, lanes),
            ],
            held.at[me, q, f],
            sem.at[q],
        )

    barrier = pltpu.get_barrier_semaphore()
    for peer in (right, left):
        pl.semaphore_signal(barrier, device_id={"row": peer}, device_id_type=MESH)
    pl.semaphore_signal(barrier, device_id={"freq": other}, device_id_type=MESH)
    order = [p * subs + k for k in range(subs) for p in range(2)]
    for q in order:
        own_copy(q, core, own_sem).start()
    lhs_copies = [
        pltpu.make_async_copy(
            m_hbm.at[c], lhs.at[0, :, pl.ds(c * block, block)], lhs_sem.at[c]
        )
        for c in range(2)
    ]
    for copy in lhs_copies:
        copy.start()
    for copy in w_copies(0):
        copy.start()
    smalls = [
        pltpu.make_async_copy(src, dst, small_sem.at[i])
        for i, (src, dst) in enumerate(
            [
                (pband_hbm, pband_v), (band_hbm, band_v), (grid_hbm, grid_v),
                (state_hbm, state_v), (freq_hbm, freq_v), (weight_hbm, weight_v),
            ]
        )
    ]
    for copy in smalls:
        copy.start()
    for q in order:
        own_copy(q, other, other_sem).start()
    pl.semaphore_wait(barrier, 3)

    for q in order:
        own_copy(q, core, own_sem).wait()
        for step in (1, 2):
            for way in (0, 1):
                first = (step + 1) % 2
                part = first if way == 0 else 1 - first
                if q // subs == part:
                    send(step * subs + q % subs, way, me, q).start()

    for copy in smalls:
        copy.wait()
    nband = band_v.shape[1]
    band_of = lax.broadcasted_iota(jnp.int32, (nband, npair), 0)
    chosen = jnp.where(band_of == pband_v[...], 1.0, 0.0).astype(jnp.bfloat16)
    pair_eps = sum(
        jnp.dot(
            jnp.broadcast_to(part, (8, nband)), chosen, preferred_element_type=jnp.float32
        )
        for part in thirds(band_v[...])
    )[:1]
    ne = grid_v.shape[1]
    spot = lax.broadcasted_iota(jnp.int32, (ne, ne), 0) == lax.broadcasted_iota(
        jnp.int32, (ne, ne), 1
    )
    energy = jnp.sum(jnp.where(spot, jnp.broadcast_to(grid_v[...], (ne, ne)), 0.0), 1, keepdims=True)
    delta = energy - pair_eps
    for j in range(nodes):
        nu = freq_v[:, j : j + 1]
        factor[j] = weight_v[:, j : j + 1] * delta / (delta * delta + nu * nu)
    state_of = lax.broadcasted_iota(jnp.int32, (NSTATE, npair), 0)
    onehot[...] = jnp.where(state_of == state_v[...], 1.0, 0.0).astype(jnp.bfloat16)
    acc[...] = jnp.zeros_like(acc)

    for copy in lhs_copies:
        copy.wait()
    lhs[1, :, :block] = -lhs[0, :, block:]
    lhs[1, :, block:] = lhs[0, :, :block]
    for q in order:
        own_copy(q, other, other_sem).wait()

    def transfers(rnd):
        got = rnd - 1

        @pl.when((got >= subs) & (got < rounds))
        def _():
            for way in (0, 1):
                owner, q = piece_of(got, way)
                send(got, way, owner, q).wait_recv()

                @pl.when(got + 2 * subs < rounds)
                def _():
                    send(got + 2 * subs, way, owner, q).start()

                pass_over(got, way, owner, q, core).start()

        done = rnd - 2

        @pl.when(done >= subs)
        def _():
            for way in (0, 1):
                owner, q = piece_of(done, way)
                pass_over(done, way, owner, q, other).wait_recv()

    def weights(rnd):
        @pl.when(rnd + 1 < rounds)
        def _():
            for copy in w_copies(rnd + 1):
                copy.start()

        for copy in w_copies(rnd):
            copy.wait()

    def multiply(rnd):
        for way in (0, 1):
            for v in range(2):
                zbuf[rnd % 2, way, v] = jnp.dot(
                    lhs[v], wbuf[rnd % 2, way], preferred_element_type=jnp.float32
                )

    def combine(rnd):
        for way in (0, 1):
            owner, q = piece_of(rnd, way)
            for f in range(2):
                for t in range(half // ROWS):
                    spots = pl.ds(t * ROWS, ROWS)
                    pairs = pl.ds(f * half + t * ROWS, ROWS)
                    r = held[owner, q, f, 0, spots, :].astype(jnp.float32)
                    s = held[owner, q, f, 1, spots, :].astype(jnp.float32)
                    for j in range(nodes):
                        zr = zbuf[rnd % 2, way, 0, pairs, j * lanes : (j + 1) * lanes]
                        zi = zbuf[rnd % 2, way, 1, pairs, j * lanes : (j + 1) * lanes]
                        re = zr * r - zi * s
                        im = zr * s + zi * r
                        acc[0, j, pairs, :] += sum(
                            re[:, i * 128 : (i + 1) * 128] for i in range(lanes // 128)
                        )
                        acc[1, j, pairs, :] += sum(
                            im[:, i * 128 : (i + 1) * 128] for i in range(lanes // 128)
                        )

    def opening(rnd, carry):
        transfers(rnd)
        weights(rnd)
        multiply(rnd)
        return carry

    def middle(rnd, carry):
        transfers(rnd)
        weights(rnd)
        combine(rnd - 2)
        multiply(rnd)
        return carry

    def closing(rnd, carry):
        transfers(rnd)
        combine(rnd - 2)
        return carry

    lax.fori_loop(0, 2, opening, 0)
    lax.fori_loop(2, rounds, middle, 0)
    lax.fori_loop(rounds, rounds + 2, closing, 0)

    line_of = lax.broadcasted_iota(jnp.int32, (lines, 3 * 128), 0)
    total = jnp.zeros((lines, half), jnp.float32)
    for c in range(2):
        for j in range(nodes):
            for f in range(2):
                parts = jnp.concatenate(thirds(acc[c, j, f * half : (f + 1) * half, :]), axis=1)
                pick = jnp.where(line_of == (c * nodes + j) * 2 + f, 1.0, 0.0).astype(jnp.bfloat16)
                total += lax.dot_general(pick, parts, NT, preferred_element_type=jnp.float32)
    forms[...] = total

    def drain(rnd, carry):
        for way in (0, 1):
            owner, q = piece_of(rnd, way)
            send(rnd, way, owner, q).wait_send()
            pass_over(rnd, way, owner, q, core).wait_send()
        return carry

    lax.fori_loop(subs, rounds, drain, 0)

    def spread(hop):
        return pltpu.make_async_remote_copy(
            src_ref=forms,
            dst_ref=peers.at[hop - 1],
            send_sem=form_send.at[hop - 1],
            recv_sem=form_recv.at[hop - 1],
            device_id={"row": (me + hop) % n},
            device_id_type=MESH,
        )

    for hop in range(1, n):
        spread(hop).start()
    total = forms[...]
    for hop in range(1, n):
        spread(hop).wait()
        total += peers[hop - 1]
    for c in range(2):
        sigma = jnp.zeros((NSTATE, ne), jnp.float32)
        for f in range(2):
            pairs = slice(f * half, (f + 1) * half)
            terms = sum(
                total[(c * nodes + j) * 2 + f : (c * nodes + j) * 2 + f + 1, :]
                * factor[j, :, pairs]
                for j in range(nodes)
            )
            for part in thirds(terms):
                sigma += lax.dot_general(
                    onehot[:, pairs], part, NT, preferred_element_type=jnp.float32
                )
        twin[0, c] = sigma
    swap = pltpu.make_async_remote_copy(
        src_ref=twin.at[0],
        dst_ref=twin.at[1],
        send_sem=twin_send,
        recv_sem=twin_recv,
        device_id={"freq": other},
        device_id_type=MESH,
    )
    swap.start()
    swap.wait()
    out_ref[...] = twin[0] + twin[1]


def ring_sigma(
    screened, elements, node_freq, node_weight, band_energy, energy_grid, pair_state, pair_band
):
    nodes = screened.shape[0]
    n = lax.axis_size("row")
    npair = elements.shape[1]
    block = elements.shape[2]
    half = npair // 2
    ne = energy_grid.shape[0]
    nband = band_energy.shape[0]
    lines = -(-4 * nodes // 8) * 8
    pieces = block // LANES
    rounds = n * pieces // 2
    dma = pltpu.SemaphoreType.DMA
    return pl.pallas_call(
        functools.partial(forms_kernel, n, nodes, npair, block, LANES, lines),
        out_shape=jax.ShapeDtypeStruct((2, NSTATE, ne), jnp.float32),
        in_specs=[pl.BlockSpec(memory_space=pl.ANY)] * 8,
        out_specs=pl.BlockSpec(memory_space=pltpu.VMEM),
        scratch_shapes=[
            pltpu.VMEM((2, npair, 2 * block), jnp.bfloat16),
            pltpu.VMEM((n, pieces, 2, 2, half, LANES), jnp.bfloat16),
            pltpu.VMEM((2, 2, 2 * block, nodes * LANES), jnp.bfloat16),
            pltpu.VMEM((2, 2, 2, npair, nodes * LANES), jnp.float32),
            pltpu.VMEM((2, nodes, npair, 128), jnp.float32),
            pltpu.VMEM((nodes, ne, npair), jnp.float32),
            pltpu.VMEM((NSTATE, npair), jnp.bfloat16),
            pltpu.VMEM((lines, half), jnp.float32),
            pltpu.VMEM((n - 1, lines, half), jnp.float32),
            pltpu.VMEM((2, 2, NSTATE, ne), jnp.float32),
            pltpu.VMEM((1, nodes), jnp.float32),
            pltpu.VMEM((1, nodes), jnp.float32),
            pltpu.VMEM((1, nband), jnp.float32),
            pltpu.VMEM((1, ne), jnp.float32),
            pltpu.VMEM((1, npair), jnp.int32),
            pltpu.VMEM((1, npair), jnp.int32),
            dma((6,)),
            dma((2,)),
            dma((pieces,)),
            dma((pieces,)),
            dma((2, 2, nodes, 2)),
            dma((rounds, 2)),
            dma((rounds, 2)),
            dma((rounds, 2)),
            dma((rounds, 2)),
            dma((n - 1,)),
            dma((n - 1,)),
            dma,
            dma,
        ],
        compiler_params=pltpu.CompilerParams(
            collective_id=0, has_side_effects=True, vmem_limit_bytes=62 * 1024 * 1024
        ),
    )(
        screened,
        elements,
        node_freq[None, :],
        node_weight[None, :],
        band_energy[None, :],
        energy_grid[None, :],
        pair_state[None, :],
        pair_band[None, :],
    )


def per_device(
    screened, elements, node_freq, node_weight, band_energy, energy_grid, pair_state, pair_band
):
    n = lax.axis_size("row")
    two = n >= 4 and n % 2 == 0 and lax.axis_size("freq") == 2
    if two and elements.shape[2] % (2 * LANES) == 0 and elements.shape[1] % (2 * ROWS) == 0:
        return ring_sigma(
            screened, elements, node_freq, node_weight, band_energy, energy_grid, pair_state,
            pair_band,
        )
    w_real = screened[:, 0]
    w_imag = screened[:, 1]
    npair = elements.shape[1]
    half = npair // lax.axis_size("freq")
    mine = lax.dynamic_slice_in_dim(elements, lax.axis_index("freq") * half, half, 1)
    collected = lax.all_gather(mine, "row", axis=2, tiled=True)
    piece = lax.all_gather(collected, "freq", axis=1, tiled=True)
    part_real = product(w_real, piece[0]) - product(w_imag, piece[1])
    part_imag = product(w_real, piece[1]) + product(w_imag, piece[0])
    stacked = jnp.stack([part_real, part_imag])
    y_real = stacked[0]
    y_imag = stacked[1]
    own_real = elements[0].T.astype(jnp.float32)[None]
    own_imag = elements[1].T.astype(jnp.float32)[None]
    form_re = jnp.sum(own_real * y_real + own_imag * y_imag, axis=1)
    form_im = jnp.sum(own_real * y_imag - own_imag * y_real, axis=1)
    form_re, form_im = lax.psum((form_re, form_im), "row")
    partial_sigma = self_energy(
        form_re, form_im, node_freq, node_weight, band_energy, energy_grid, pair_state, pair_band
    )
    return lax.psum(partial_sigma, "freq")


def solution(mesh):
    in_specs = (
        P(("kpt", "freq"), None, "row", None),
        P(None, "kpt", "row"),
        P("freq"),
        P("freq"),
        P("kpt"),
        P(),
        P("kpt"),
        P("kpt"),
    )
    out_specs = P(None, "kpt", None)
    return jax.shard_map(
        per_device, mesh=mesh, in_specs=in_specs, out_specs=out_specs, check_vma=False
    )
```

```python
import functools

import jax
import jax.numpy as jnp
from jax import lax
from jax.experimental import pallas as pl
from jax.experimental.pallas import tpu as pltpu
from jax.sharding import PartitionSpec as P

NSTATE = 32
LANES = 256
ROWS = 32
MESH = pl.DeviceIdType.MESH
NT = (((1,), (1,)), ((), ()))


def product(weights, piece):
    return jnp.einsum("jgc,pc->jgp", weights, piece, preferred_element_type=jnp.float32)


def self_energy(
    form_re, form_im, node_freq, node_weight, band_energy, energy_grid, pair_state, pair_band
):
    band_onehot = (
        pair_band[:, None] == jnp.arange(band_energy.shape[0], dtype=jnp.int32)[None, :]
    ).astype(jnp.float32)
    pair_eps = jnp.dot(band_onehot, band_energy, precision=lax.Precision.HIGHEST)
    delta = energy_grid[None, :] - pair_eps[:, None]
    factor = (
        node_weight[:, None, None]
        * delta[None]
        / (delta[None] ** 2 + node_freq[:, None, None] ** 2)
    )
    terms_re = jnp.sum(form_re[:, :, None] * factor, axis=0)
    terms_im = jnp.sum(form_im[:, :, None] * factor, axis=0)
    state_onehot = (jnp.arange(NSTATE, dtype=jnp.int32)[:, None] == pair_state[None, :]).astype(
        jnp.float32
    )
    sig_re = jnp.dot(state_onehot, terms_re, precision=lax.Precision.HIGHEST)
    sig_im = jnp.dot(state_onehot, terms_im, precision=lax.Precision.HIGHEST)
    return jnp.stack([sig_re, sig_im])


def ring_position(idx, n):
    par = idx % 2
    return (1 - par) * (idx // 2) + par * (n - 1 - idx // 2)


def ring_index(pos, n):
    high = pos // (n // 2)
    return (1 - high) * (2 * pos) + high * (2 * (n - 1 - pos) + 1)


def thirds(x):
    high = x.astype(jnp.bfloat16)
    rest = x - high.astype(jnp.float32)
    mid = rest.astype(jnp.bfloat16)
    low = (rest - mid.astype(jnp.float32)).astype(jnp.bfloat16)
    return high, mid, low


def forms_kernel(
    n, nodes, npair, block, lanes, lines,
    w_hbm, m_hbm, freq_hbm, weight_hbm, band_hbm, grid_hbm, state_hbm, pband_hbm,
    out_ref,
    neg, held, wbuf, zbuf, acc, factor, onehot, forms, peers, twin,
    freq_v, weight_v, band_v, grid_v, state_v, pband_v,
    small_sem, own_sem, other_sem, w_sem,
    send_sem, recv_sem, sib_send, sib_recv, form_send, form_recv, twin_send, twin_recv,
):
    me = lax.axis_index("row")
    core = lax.axis_index("freq")
    pos = ring_position(me, n)
    right = ring_index((pos + 1) % n, n)
    left = ring_index((pos + n - 1) % n, n)
    other = 1 - core
    half = npair // 2
    subs = block // lanes // 2
    rounds = n * subs

    def item(step, way, hop):
        first = (step + 1) % 2
        owner_pos = (pos + n + (2 * way - 1) * hop) % n
        part = (1 - way) * first + way * (1 - first)
        return ring_index(owner_pos, n), part

    def piece_of(rnd, way):
        step = rnd // subs
        owner, part = item(step, way, (step + 1) // 2)
        return owner, part * subs + rnd % subs

    def w_copies(rnd):
        copies = []
        for way in range(2):
            owner, q = piece_of(rnd, way)
            start = pl.multiple_of(owner * block + q * lanes, 128)
            for j in range(nodes):
                for c in range(2):
                    copies.append(
                        pltpu.make_async_copy(
                            w_hbm.at[j, c, :, pl.ds(start, lanes)],
                            wbuf.at[rnd % 2, way, pl.ds(c * block, block), pl.ds(j * lanes, lanes)],
                            w_sem.at[rnd % 2, way, j, c],
                        )
                    )
        return copies

    def send(rnd, way, owner, q):
        ref = held.at[owner, q, core]
        return pltpu.make_async_remote_copy(
            src_ref=ref,
            dst_ref=ref,
            send_sem=send_sem.at[rnd, way],
            recv_sem=recv_sem.at[rnd, way],
            device_id={"row": right if way == 0 else left},
            device_id_type=MESH,
        )

    def pass_over(rnd, way, owner, q, core_of):
        ref = held.at[owner, q, core_of]
        return pltpu.make_async_remote_copy(
            src_ref=ref,
            dst_ref=ref,
            send_sem=sib_send.at[rnd, way],
            recv_sem=sib_recv.at[rnd, way],
            device_id={"freq": other},
            device_id_type=MESH,
        )

    def own_copy(q, f, sem):
        return pltpu.make_async_copy(
            m_hbm.at[
                :,
                pl.ds(pl.multiple_of(f * half, half), half),
                pl.ds(q * lanes, lanes),
            ],
            held.at[me, q, f],
            sem.at[q],
        )

    barrier = pltpu.get_barrier_semaphore()
    for peer in (right, left):
        pl.semaphore_signal(barrier, device_id={"row": peer}, device_id_type=MESH)
    pl.semaphore_signal(barrier, device_id={"freq": other}, device_id_type=MESH)
    order = [p * subs + k for k in range(subs) for p in range(2)]
    for q in order:
        own_copy(q, core, own_sem).start()
    for q in order:
        own_copy(q, other, other_sem).start()
    smalls = [
        pltpu.make_async_copy(src, dst, small_sem.at[i])
        for i, (src, dst) in enumerate(
            [
                (pband_hbm, pband_v), (band_hbm, band_v), (grid_hbm, grid_v),
                (state_hbm, state_v), (freq_hbm, freq_v), (weight_hbm, weight_v),
            ]
        )
    ]
    for copy in smalls:
        copy.start()
    for copy in w_copies(0):
        copy.start()
    pl.semaphore_wait(barrier, 3)

    for q in order:
        own_copy(q, core, own_sem).wait()
        send(subs + q % subs, q // subs, me, q).start()

    for copy in smalls:
        copy.wait()
    nband = band_v.shape[1]
    band_of = lax.broadcasted_iota(jnp.int32, (nband, npair), 0)
    chosen = jnp.where(band_of == pband_v[...], 1.0, 0.0).astype(jnp.bfloat16)
    pair_eps = sum(
        jnp.dot(
            jnp.broadcast_to(part, (8, nband)), chosen, preferred_element_type=jnp.float32
        )
        for part in thirds(band_v[...])
    )[:1]
    ne = grid_v.shape[1]
    spot = lax.broadcasted_iota(jnp.int32, (ne, ne), 0) == lax.broadcasted_iota(
        jnp.int32, (ne, ne), 1
    )
    energy = jnp.sum(jnp.where(spot, jnp.broadcast_to(grid_v[...], (ne, ne)), 0.0), 1, keepdims=True)
    delta = energy - pair_eps
    for j in range(nodes):
        nu = freq_v[:, j : j + 1]
        factor[j] = weight_v[:, j : j + 1] * delta / (delta * delta + nu * nu)
    state_of = lax.broadcasted_iota(jnp.int32, (NSTATE, npair), 0)
    onehot[...] = jnp.where(state_of == state_v[...], 1.0, 0.0).astype(jnp.bfloat16)
    acc[...] = jnp.zeros_like(acc)

    for q in order:
        own_copy(q, other, other_sem).wait()
    for q in range(2 * subs):
        for f in range(2):
            neg[q, f] = -held[me, q, f, 1]

    def transfers(rnd):
        got = rnd - 1

        @pl.when((got >= subs) & (got < rounds))
        def _():
            for way in (0, 1):
                owner, q = piece_of(got, way)
                send(got, way, owner, q).wait_recv()
                pass_over(got, way, owner, q, core).start()

        @pl.when((got >= 0) & (got + 2 * subs < rounds))
        def _():
            for way in (0, 1):
                owner, q = piece_of(got, way)
                send(got + 2 * subs, way, owner, q).start()

        done = rnd - 2

        @pl.when(done >= subs)
        def _():
            for way in (0, 1):
                owner, q = piece_of(done, way)
                pass_over(done, way, owner, q, other).wait_recv()

    def prefetch(rnd):
        @pl.when(rnd + 1 < rounds)
        def _():
            for copy in w_copies(rnd + 1):
                copy.start()

    def multiply(rnd, way, v, f):
        total = 0.0
        for c in range(2):
            for q in range(2 * subs):
                left_side = neg[q, f] if (v, c) == (1, 0) else held[me, q, f, c * (1 - v)]
                right_side = wbuf[rnd % 2, way, pl.ds(c * block + q * lanes, lanes)]
                total += jnp.dot(left_side, right_side, preferred_element_type=jnp.float32)
        zbuf[rnd % 3, way, v, pl.ds(f * half, half)] = total

    def combine(rnd, f, t):
        slot = rnd % 3
        spots = pl.ds(t * ROWS, ROWS)
        pairs = pl.ds(f * half + t * ROWS, ROWS)
        sums = [[0.0] * nodes for _ in range(2)]
        for way in (0, 1):
            owner, q = piece_of(rnd, way)
            for i in range(lanes // 128):
                cut = slice(i * 128, (i + 1) * 128)
                r = held[owner, q, f, 0, spots, cut].astype(jnp.float32)
                s = held[owner, q, f, 1, spots, cut].astype(jnp.float32)
                for j in range(nodes):
                    cut = slice(j * lanes + i * 128, j * lanes + (i + 1) * 128)
                    zr = zbuf[slot, way, 0, pairs, cut]
                    zi = zbuf[slot, way, 1, pairs, cut]
                    sums[0][j] += zr * r - zi * s
                    sums[1][j] += zr * s + zi * r
        for j in range(nodes):
            acc[0, j, pairs, :] += sums[0][j]
            acc[1, j, pairs, :] += sums[1][j]

    tiles = [
        (way, v, f) for way in (0, 1) for f in range(2) for v in range(2)
    ]
    strips = [(f, t) for f in range(2) for t in range(half // ROWS)]

    def opening(rnd, carry):
        transfers(rnd)
        prefetch(rnd)
        copies = w_copies(rnd)
        each = len(copies) // 2
        for way in (0, 1):
            for copy in copies[way * each : (way + 1) * each]:
                copy.wait()
            for tile in tiles:
                if tile[0] == way:
                    multiply(rnd, *tile)
        return carry

    def middle(rnd, carry):
        transfers(rnd)
        prefetch(rnd)
        for copy in w_copies(rnd):
            copy.wait()
        for i, tile in enumerate(tiles):
            multiply(rnd, *tile)
            for strip in strips[i * len(strips) // len(tiles) : (i + 1) * len(strips) // len(tiles)]:
                combine(rnd - 2, *strip)
        return carry

    def closing(rnd, carry):
        transfers(rnd)
        for strip in strips:
            combine(rnd - 2, *strip)
        return carry

    lax.fori_loop(0, 2, opening, 0)
    lax.fori_loop(2, rounds, middle, 0)
    lax.fori_loop(rounds, rounds + 2, closing, 0)

    line_of = lax.broadcasted_iota(jnp.int32, (lines, 2 * 128), 0)
    total = jnp.zeros((lines, half), jnp.float32)
    for c in range(2):
        for j in range(nodes):
            for f in range(2):
                parts = jnp.concatenate(thirds(acc[c, j, f * half : (f + 1) * half, :])[:2], axis=1)
                pick = jnp.where(line_of == (c * nodes + j) * 2 + f, 1.0, 0.0).astype(jnp.bfloat16)
                total += lax.dot_general(pick, parts, NT, preferred_element_type=jnp.float32)
    forms[...] = total

    def spread(hop):
        return pltpu.make_async_remote_copy(
            src_ref=forms,
            dst_ref=peers.at[hop - 1],
            send_sem=form_send.at[hop - 1],
            recv_sem=form_recv.at[hop - 1],
            device_id={"row": (me + hop) % n},
            device_id_type=MESH,
        )

    for hop in range(1, n):
        spread(hop).start()

    def drain(rnd, carry):
        for way in (0, 1):
            owner, q = piece_of(rnd, way)
            send(rnd, way, owner, q).wait_send()
            pass_over(rnd, way, owner, q, core).wait_send()
        return carry

    lax.fori_loop(subs, rounds, drain, 0)
    total = forms[...]
    for hop in range(1, n):
        spread(hop).wait()
        total += peers[hop - 1]
    for c in range(2):
        sigma = jnp.zeros((NSTATE, ne), jnp.float32)
        for f in range(2):
            pairs = slice(f * half, (f + 1) * half)
            terms = sum(
                total[(c * nodes + j) * 2 + f : (c * nodes + j) * 2 + f + 1, :]
                * factor[j, :, pairs]
                for j in range(nodes)
            )
            for part in thirds(terms):
                sigma += lax.dot_general(
                    onehot[:, pairs], part, NT, preferred_element_type=jnp.float32
                )
        twin[0, c] = sigma
    swap = pltpu.make_async_remote_copy(
        src_ref=twin.at[0],
        dst_ref=twin.at[1],
        send_sem=twin_send,
        recv_sem=twin_recv,
        device_id={"freq": other},
        device_id_type=MESH,
    )
    swap.start()
    swap.wait()
    out_ref[...] = twin[0] + twin[1]


def ring_sigma(
    screened, elements, node_freq, node_weight, band_energy, energy_grid, pair_state, pair_band
):
    nodes = screened.shape[0]
    n = lax.axis_size("row")
    npair = elements.shape[1]
    block = elements.shape[2]
    half = npair // 2
    ne = energy_grid.shape[0]
    nband = band_energy.shape[0]
    lines = -(-4 * nodes // 8) * 8
    pieces = block // LANES
    rounds = n * pieces // 2
    dma = pltpu.SemaphoreType.DMA
    return pl.pallas_call(
        functools.partial(forms_kernel, n, nodes, npair, block, LANES, lines),
        out_shape=jax.ShapeDtypeStruct((2, NSTATE, ne), jnp.float32),
        in_specs=[pl.BlockSpec(memory_space=pl.ANY)] * 8,
        out_specs=pl.BlockSpec(memory_space=pltpu.VMEM),
        scratch_shapes=[
            pltpu.VMEM((pieces, 2, half, LANES), jnp.bfloat16),
            pltpu.VMEM((n, pieces, 2, 2, half, LANES), jnp.bfloat16),
            pltpu.VMEM((2, 2, 2 * block, nodes * LANES), jnp.bfloat16),
            pltpu.VMEM((3, 2, 2, npair, nodes * LANES), jnp.float32),
            pltpu.VMEM((2, nodes, npair, 128), jnp.float32),
            pltpu.VMEM((nodes, ne, npair), jnp.float32),
            pltpu.VMEM((NSTATE, npair), jnp.bfloat16),
            pltpu.VMEM((lines, half), jnp.float32),
            pltpu.VMEM((n - 1, lines, half), jnp.float32),
            pltpu.VMEM((2, 2, NSTATE, ne), jnp.float32),
            pltpu.VMEM((1, nodes), jnp.float32),
            pltpu.VMEM((1, nodes), jnp.float32),
            pltpu.VMEM((1, nband), jnp.float32),
            pltpu.VMEM((1, ne), jnp.float32),
            pltpu.VMEM((1, npair), jnp.int32),
            pltpu.VMEM((1, npair), jnp.int32),
            dma((6,)),
            dma((pieces,)),
            dma((pieces,)),
            dma((2, 2, nodes, 2)),
            dma((rounds, 2)),
            dma((rounds, 2)),
            dma((rounds, 2)),
            dma((rounds, 2)),
            dma((n - 1,)),
            dma((n - 1,)),
            dma,
            dma,
        ],
        compiler_params=pltpu.CompilerParams(
            collective_id=0, has_side_effects=True, vmem_limit_bytes=62 * 1024 * 1024
        ),
    )(
        screened,
        elements,
        node_freq[None, :],
        node_weight[None, :],
        band_energy[None, :],
        energy_grid[None, :],
        pair_state[None, :],
        pair_band[None, :],
    )


def per_device(
    screened, elements, node_freq, node_weight, band_energy, energy_grid, pair_state, pair_band
):
    n = lax.axis_size("row")
    two = n >= 4 and n % 2 == 0 and lax.axis_size("freq") == 2
    if two and elements.shape[2] % (2 * LANES) == 0 and elements.shape[1] % (2 * ROWS) == 0:
        return ring_sigma(
            screened, elements, node_freq, node_weight, band_energy, energy_grid, pair_state,
            pair_band,
        )
    w_real = screened[:, 0]
    w_imag = screened[:, 1]
    npair = elements.shape[1]
    half = npair // lax.axis_size("freq")
    mine = lax.dynamic_slice_in_dim(elements, lax.axis_index("freq") * half, half, 1)
    collected = lax.all_gather(mine, "row", axis=2, tiled=True)
    piece = lax.all_gather(collected, "freq", axis=1, tiled=True)
    part_real = product(w_real, piece[0]) - product(w_imag, piece[1])
    part_imag = product(w_real, piece[1]) + product(w_imag, piece[0])
    stacked = jnp.stack([part_real, part_imag])
    y_real = stacked[0]
    y_imag = stacked[1]
    own_real = elements[0].T.astype(jnp.float32)[None]
    own_imag = elements[1].T.astype(jnp.float32)[None]
    form_re = jnp.sum(own_real * y_real + own_imag * y_imag, axis=1)
    form_im = jnp.sum(own_real * y_imag - own_imag * y_real, axis=1)
    form_re, form_im = lax.psum((form_re, form_im), "row")
    partial_sigma = self_energy(
        form_re, form_im, node_freq, node_weight, band_energy, energy_grid, pair_state, pair_band
    )
    return lax.psum(partial_sigma, "freq")


def solution(mesh):
    in_specs = (
        P(("kpt", "freq"), None, "row", None),
        P(None, "kpt", "row"),
        P("freq"),
        P("freq"),
        P("kpt"),
        P(),
        P("kpt"),
        P("kpt"),
    )
    out_specs = P(None, "kpt", None)
    return jax.shard_map(
        per_device, mesh=mesh, in_specs=in_specs, out_specs=out_specs, check_vma=False
    )
```
